32 devices in a mesh: strip: 8 (over z, y), chan: 4 (over x, core).
Axes of the slice: x: 2, y: 2, z: 4, core: 2. Of those that a mesh axis runs over, the one named last changes fastest.
Arguments:
- activations: bfloat16 [64, 128, 1280], P('strip', None, 'chan'), may hold values from -17 to 17
- weight: bfloat16 [9, 1280, 1280], P(None, None, 'chan'), may hold values from -0.0546875 to 0.0546875
- gamma: float32 [1280], replicated, may hold values from 0.25 to 1.75
- beta: float32 [1280], replicated, may hold values from -3 to 3
- group_map: int32 [1280], replicated, may hold values from 0 to 31, as said below
- lengths: int32 [8], P('strip'), may hold values from 1 to 8, 48 in all
- stale_edges: bfloat16 [16, 128, 1280], P('strip', None, 'chan'), may hold values from -6 to 6
- stale_mean: float32 [32], replicated, may hold values from -0.5 to 0.5
- stale_square: float32 [32], replicated, may hold values from 1 to 4
- old_mean: float32 [8, 32], P('strip'), may hold values from -0.5 to 0.5
- old_square: float32 [8, 32], P('strip'), may hold values from 0.5 to 6
Outputs:
- upsampled: bfloat16 [128, 256, 1280], P('strip', None, 'chan')
- new_mean: float32 [32], replicated
- new_square: float32 [32], replicated
The draws below stay inside these ranges and needn't reach their ends.
Inputs may be any that keep to these rules, and one draw needn't show every extreme that they name: `group_map`: every group has exactly 40 channels. The lengths sum to 48, and some strip uses all 8 rows.
All inputs are finite; a program needn't handle non-finite values. No bound on the sum of `lengths` on one device may be relied on, other than what follows from the above.
Results may differ from the reference program's by a relative error of at most 0.0027.
Values may be sent and summed in bfloat16 or wider, within the bound.
No kernel may reach another device: no remote copies, remote signals or barrier semaphores. Data moves between devices by JAX's collectives and lax.ppermute only.
A program may use at most 64 MiB of HBM per device.

```python
import math
import jax
import jax.numpy as jnp
import numpy as np
from jax import lax

C = 1280
G = 32
ROWS_DEV = 8
WIDTH = 128
HEIGHT = 64
N_STRIP = 8


def draw_activations(key, part):
    first, second = jax.random.split(key, 2)
    position = jnp.arange(HEIGHT, dtype=jnp.float32) / (HEIGHT - 1)
    noise = jnp.clip(jax.random.normal(first, (HEIGHT, WIDTH, C), jnp.float32), -5.0, 5.0)
    offset = jax.random.uniform(second, (C,), jnp.float32, -1.0, 1.0)
    spread = 1.0 + 2.0 * position
    return (noise * spread[:, None, None] + offset[None, None, :]).astype(jnp.bfloat16)


def draw_group_map(key, part):
    order = jax.random.permutation(key, C)
    return (order // (C // G)).astype(jnp.int32)


def steps_of(rng, shape, cuts, low, top_value):
    level, own = 1.0, jax.random.fold_in(rng, 6)
    for axis_at, blocks in cuts:
        draws = jnp.exp(jax.random.uniform(jax.random.fold_in(own, axis_at), (blocks,), jnp.float32, low / len(cuts), top_value / len(cuts)))
        level = level * jnp.repeat(draws, shape[axis_at] // blocks).reshape([-1 if axis == axis_at else 1 for axis in range(len(shape))])
    return level


def length_profile(count, total, bound, slope):
    loads = [(1 << 20) // math.isqrt(standing ** slope) + 1 for standing in range(2, count + 1)]
    surplus, counts = total - bound - (count - 1), [1] * (count - 1)
    while surplus > 0:
        free = [i for i in range(count - 1) if counts[i] < bound]
        pool, remaining = sum([loads[i] for i in free]), surplus
        for i in free:
            extra = min(bound - counts[i], max(1, remaining * loads[i] // pool), surplus)
            counts[i] = counts[i] + extra
            surplus = surplus - extra
    return np.array([bound] + counts)


def uneven_parts(own_key, amount, total, most, lean):
    if amount == 2:
        one = jax.random.randint(own_key, (), max(1, total - most), min(most, total - 1) + 1)
        return jnp.stack([one, total - one])
    sizes = jnp.asarray(length_profile(amount, total, most, lean), jnp.int32)
    pairs = (amount - 1) // 2
    donor, taker = sizes[1:1 + 2 * pairs:2], sizes[2:2 + 2 * pairs:2]
    margin = jnp.minimum(donor - 1, most - taker)
    shifted = jax.random.randint(jax.random.fold_in(own_key, 1), (pairs,), 0, 1 << 20) % (margin + 1)
    sizes = sizes.at[1:1 + 2 * pairs:2].set(donor - shifted).at[2:2 + 2 * pairs:2].set(taker + shifted)
    return sizes[jax.random.permutation(jax.random.fold_in(own_key, 2), amount)]


def scatter_about(stream_key, extent, scale, bound, pieces=(), kind=jnp.bfloat16):
    drawn = scale * jax.random.normal(stream_key, extent, jnp.float32)
    if pieces:
        drawn = drawn * steps_of(stream_key, extent, pieces, -0.22, 0.18)
    return jnp.clip(drawn, -bound, bound).astype(kind)


def setup_inputs(seed: int = 0) -> dict:
    seeds = jax.random.split(jax.random.key(seed), 12)
    return {
        "activations": draw_activations(jax.random.fold_in(seeds[11], 71), 0),
        "weight": scatter_about(seeds[1], (9, C, C), (9 * C) ** -0.5, 0.0546875, ((2, 4),)),
        "gamma": jnp.clip(1.0 + 0.15 * jax.random.normal(seeds[2], (C,), jnp.float32), 0.25, 1.75),
        "beta": scatter_about(seeds[3], (C,), 0.7, 3.0, (), jnp.float32),
        "group_map": draw_group_map(jax.random.fold_in(seeds[11], 71), 0),
        "lengths": uneven_parts(seeds[5], N_STRIP, N_STRIP * (3 * ROWS_DEV // 4), ROWS_DEV, 2).astype(jnp.int32),
        "stale_edges": scatter_about(seeds[6], (2 * N_STRIP, WIDTH, C), 1.0, 6.0, ((0, 8), (2, 4))),
        "stale_mean": jnp.clip(jax.random.uniform(seeds[7], (G,), jnp.float32, -0.5, 0.5), -0.5, 0.5),
        "stale_square": jnp.clip(jax.random.uniform(seeds[8], (G,), jnp.float32, 1.0, 4.0), 1.0, 4.0),
        "old_mean": jnp.clip(jax.random.uniform(seeds[9], (N_STRIP, G), jnp.float32, -0.5, 0.5) * steps_of(seeds[9], (N_STRIP, G), ((0, 8),), -0.4, 0.0), -0.5, 0.5),
        "old_square": jnp.clip(0.5 + 5.5 * jax.random.uniform(seeds[10], (N_STRIP, G), jnp.float32) ** steps_of(seeds[10], (N_STRIP, G), ((0, 8),), -0.2, 0.2), 0.5, 6.0),
    }


EPS = 1e-05

def reference(activations, weight, gamma, beta, group_map, lengths, stale_edges, stale_mean, stale_square, old_mean, old_square):
    per_group = C // G
    grid = activations.reshape(N_STRIP, ROWS_DEV, WIDTH, C)
    member = (group_map[:, None] == jnp.arange(G, dtype=jnp.int32)[None, :]).astype(jnp.float32)
    used = (jnp.arange(ROWS_DEV, dtype=jnp.int32)[None, :] < lengths[:, None]).astype(jnp.float32)
    values = grid.astype(jnp.float32) * used[:, :, None, None]
    chan_sum = lax.optimization_barrier(jnp.sum(values, axis=(1, 2)))
    chan_sq = lax.optimization_barrier(jnp.sum(values * values, axis=(1, 2)))
    sum_one = lax.optimization_barrier(jnp.sum(chan_sum[:, :, None] * member[None], axis=1))
    sum_two = lax.optimization_barrier(jnp.sum(chan_sq[:, :, None] * member[None], axis=1))
    count = (lengths.astype(jnp.float32) * (WIDTH * per_group))[:, None]
    fresh_mean = sum_one / count
    fresh_square = sum_two / count
    mean_g = stale_mean[None] + fresh_mean - old_mean
    square_g = stale_square[None] + fresh_square - old_square
    var_g = jnp.maximum(square_g - mean_g * mean_g, 0.5 * (fresh_square - fresh_mean * fresh_mean))
    rstd_g = lax.rsqrt(var_g + EPS)
    scale_c = lax.optimization_barrier(jnp.sum(member[None] * rstd_g[:, None, :], axis=2)) * gamma[None]
    shift_c = beta[None] - lax.optimization_barrier(jnp.sum(member[None] * mean_g[:, None, :], axis=2)) * scale_c
    edges = stale_edges.reshape(N_STRIP, 2, WIDTH, C)
    zero_row = jnp.zeros((1, WIDTH, C), jnp.bfloat16)
    upper = jnp.concatenate([zero_row, edges[:-1, 1]], axis=0)
    lower = jnp.concatenate([edges[1:, 0], zero_row], axis=0)

    def one_strip(items):
        strip_x, scale, shift, mask, above, below, length = items
        maskb = mask[:, None, None]
        act = (jax.nn.silu(strip_x.astype(jnp.float32) * scale + shift) * maskb).astype(jnp.bfloat16)
        padded = jnp.concatenate([above[None], act, jnp.zeros((1, WIDTH, C), jnp.bfloat16)], axis=0)
        place = (jnp.arange(ROWS_DEV + 2, dtype=jnp.int32) == length + 1)[:, None, None]
        padded = jnp.where(place, below[None], padded)
        padded = jnp.pad(padded, ((0, 0), (1, 1), (0, 0)))
        total = jnp.zeros((ROWS_DEV * WIDTH, C), jnp.float32)
        for tap in range(9):
            dy, dx = (tap // 3, tap % 3)
            patch = padded[dy:dy + ROWS_DEV, dx:dx + WIDTH].reshape(ROWS_DEV * WIDTH, C)
            total = total + jnp.dot(patch, weight[tap], preferred_element_type=jnp.float32)
        block = (strip_x.astype(jnp.float32) + total.reshape(ROWS_DEV, WIDTH, C)) * maskb
        return block.astype(jnp.bfloat16)
    blocks = lax.map(one_strip, (grid, scale_c, shift_c, used, upper, lower, lengths))
    blocks = blocks.reshape(HEIGHT, WIDTH, C)
    upsampled = jnp.repeat(jnp.repeat(blocks, 2, axis=0), 2, axis=1)
    total_count = float(N_STRIP * (3 * ROWS_DEV // 4) * WIDTH * per_group)
    new_mean = lax.optimization_barrier(jnp.sum(sum_one, axis=0)) / total_count
    new_square = lax.optimization_barrier(jnp.sum(sum_two, axis=0)) / total_count
    return (upsampled, new_mean, new_square)
```

```python
import functools

import jax
import jax.numpy as jnp
from jax import lax
from jax.experimental import pallas as pl
from jax.experimental.pallas import tpu as pltpu
from jax.sharding import PartitionSpec as P


EPS = 1e-05
EARLY = 4
HI = lax.Precision.HIGHEST
VMEM = pltpu.VMEM
MIB = 1 << 20


def spec(space=VMEM):
    return pl.BlockSpec(memory_space=space)


def to_column(row):
    n = row.shape[1]
    same = lax.broadcasted_iota(jnp.int32, (n, n), 0) == lax.broadcasted_iota(jnp.int32, (n, n), 1)
    return jnp.sum(jnp.where(same, row, 0.0), axis=1, keepdims=True)


def to_row(column):
    n = column.shape[0]
    same = lax.broadcasted_iota(jnp.int32, (n, n), 0) == lax.broadcasted_iota(jnp.int32, (n, n), 1)
    return jnp.sum(jnp.where(same, column, 0.0), axis=0, keepdims=True)


def lane(sums, at):
    lanes = lax.broadcasted_iota(jnp.int32, sums.shape, 1)
    return jnp.sum(jnp.where(lanes == at, sums, 0.0), axis=1, keepdims=True)


def split(sums):
    first = sums.astype(jnp.bfloat16)
    rest = sums - first.astype(jnp.float32)
    second = rest.astype(jnp.bfloat16)
    third = (rest - second.astype(jnp.float32)).astype(jnp.bfloat16)
    return first, second, third


def put_sums(ref, row, sums):
    n = sums.shape[0]
    for i, piece in enumerate(split(sums)):
        ref[row, i * n : (i + 1) * n, :] = piece


def get_sums(ref, row, n):
    pieces = [ref[row, i * n : (i + 1) * n, :].astype(jnp.float32) for i in range(3)]
    return pieces[0] + (pieces[1] + pieces[2])


def stats_kernel(
    n_chan, groups, where_ref, gm_ref, x_ref, edge_ref, head_ref, tail_ref, near_ref, part_ref, in_ref, s_ref, sems
):
    rows, local_c, width = x_ref.shape
    length, me, odd = where_ref[0], where_ref[1], where_ref[2]
    early = head_ref.shape[0] - 1
    copies = [
        pltpu.make_async_copy(x_ref, in_ref, sems.at[0]),
        pltpu.make_async_copy(edge_ref.at[1 - odd], near_ref.at[0], sems.at[1]),
    ]
    for copy in copies:
        copy.start()
    copies[0].wait()
    step = 64
    for at in range(0, local_c, step):
        one = jnp.zeros((step, width), jnp.float32)
        two = jnp.zeros((step, width), jnp.float32)
        for r in range(rows):
            value = in_ref[r, at : at + step, :]
            if r < early:
                head_ref[r, at : at + step, :] = value
            else:
                tail_ref[r - early, at : at + step, :] = value
            value = jnp.where(r < length, value.astype(jnp.float32), 0.0)
            one = one + value
            two = two + value * value
        s_ref[at : at + step, :width] = one
        s_ref[at : at + step, width:] = two
    mine = gm_ref[:, :local_c]
    for k in range(1, n_chan):
        mine = jnp.where(me == k, gm_ref[:, k * local_c : (k + 1) * local_c], mine)
    member = (lax.broadcasted_iota(jnp.int32, (groups, local_c), 0) == mine).astype(jnp.float32)
    sums = jnp.dot(member, s_ref[...], precision=HI, preferred_element_type=jnp.float32)
    one = jnp.sum(sums[:, :width], axis=1, keepdims=True)
    two = jnp.sum(sums[:, width:], axis=1, keepdims=True)
    lanes = lax.broadcasted_iota(jnp.int32, part_ref.shape, 1)
    part = jnp.where(lanes == 0, one, jnp.where(lanes == 1, two, 0.0))
    part_ref[...] = part
    put_sums(head_ref, early, part)
    put_sums(near_ref, 1, part)
    copies[1].wait()


def far_kernel(where_ref, near_ref, part_ref, edge_ref, far_ref, pair_ref, sem):
    copy = pltpu.make_async_copy(edge_ref.at[where_ref[2]], far_ref.at[0], sem)
    copy.start()
    pair = part_ref[...] + get_sums(near_ref, 1, part_ref.shape[0])
    pair_ref[...] = pair
    put_sums(far_ref, 1, pair)
    copy.wait()


def halo_kernel(where_ref, near_ref, far_ref, mine_ref, other_ref, out_ref):
    odd, strip, n_strip = where_ref[2], where_ref[3], where_ref[4]
    near, far = near_ref[0], far_ref[0]
    above = jnp.where(odd == 1, near, far)
    below = jnp.where(odd == 1, far, near)
    zero = jnp.zeros_like(near)
    out_ref[0] = jnp.where(strip == 0, zero, above)
    out_ref[1] = jnp.where(strip == n_strip - 1, zero, below)
    put_sums(out_ref, 2, mine_ref[...] + other_ref[...])


def conv_kernel(
    n_chan,
    per_group,
    total,
    where_ref,
    part_ref,
    smean_ref,
    ssquare_ref,
    omean_ref,
    osquare_ref,
    gm_ref,
    gamma_ref,
    beta_ref,
    *refs,
):
    x_any, w_any, refs = refs[0], refs[1], refs[2:]
    m_refs, refs = (None,) + refs[: n_chan - 1], refs[n_chan - 1 :]
    t_refs, refs = (None,) + refs[: n_chan - 1], refs[n_chan - 1 :]
    h_refs, refs = refs[:n_chan], refs[n_chan:]
    out_ref, mean_ref, square_ref, x_ref, w_ref, a_ref, ss_ref, o_ref, sem, sems = refs
    rows, local_c, width = x_ref.shape
    early = m_refs[1].shape[0] - 1
    copies = [pltpu.make_async_copy(x_any, x_ref, sems.at[0])]
    for dy in range(3):
        copies.append(pltpu.make_async_copy(w_any.at[dy], w_ref.at[dy], sems.at[1 + dy]))
    for copy in copies:
        copy.start()

    def source(k, r):
        if k == 0:
            return x_ref, r
        return (m_refs[k], r) if r < early else (t_refs[k], r - early)

    channels = n_chan * local_c
    groups = smean_ref.shape[1]
    length, me = where_ref[0], where_ref[1]
    image = get_sums(h_refs[0], 2, groups)
    strip = part_ref[...]
    for k in range(1, n_chan):
        image = image + get_sums(h_refs[k], 2, groups)
        strip = strip + get_sums(m_refs[k], early, groups)
    mean_ref[...] = to_row(lane(image, 0)) / total
    square_ref[...] = to_row(lane(image, 1)) / total

    count = length.astype(jnp.float32) * (width * per_group)
    count = jnp.full((groups, 1), count, jnp.float32)
    fresh_mean = lane(strip, 0) / count
    fresh_square = lane(strip, 1) / count
    mean = to_column(smean_ref[...]) + fresh_mean - to_column(omean_ref[...])
    square = to_column(ssquare_ref[...]) + fresh_square - to_column(osquare_ref[...])
    var = jnp.maximum(square - mean * mean, 0.5 * (fresh_square - fresh_mean * fresh_mean))
    rstd = lax.rsqrt(var + EPS)
    member = lax.broadcasted_iota(jnp.int32, (groups, channels), 0) == gm_ref[...]
    left = jnp.where(member, gamma_ref[...], 0.0)
    first = lax.broadcasted_iota(jnp.int32, (8, channels), 0) == 0
    left = jnp.concatenate([left, jnp.where(first, beta_ref[...], 0.0)], axis=0)
    ones = (lax.broadcasted_iota(jnp.int32, (8, width), 0) == 0).astype(jnp.float32)
    right = jnp.concatenate(
        [
            jnp.concatenate([jnp.broadcast_to(rstd, (groups, width)), jnp.broadcast_to(-mean * rstd, (groups, width))], axis=1),
            jnp.concatenate([jnp.zeros_like(ones), ones], axis=1),
        ],
        axis=0,
    )
    ss_ref[...] = lax.dot_general(
        left, right, (((0,), (0,)), ((), ())), precision=HI, preferred_element_type=jnp.float32
    )

    zero = jnp.zeros((channels, width), jnp.bfloat16)
    a_ref[rows + 1] = zero
    copies[0].wait()
    for k in range(n_chan):
        owner = jnp.bitwise_xor(me, k)
        base = pl.multiple_of(owner * local_c, 64)
        a_ref[0, pl.ds(base, local_c), :] = h_refs[k][0]
        step = 64
        for at in range(0, local_c, step):
            here = pl.ds(pl.multiple_of(base + at, 64), step)
            scale = ss_ref[here, :width]
            shift = ss_ref[here, width:]
            for r in range(rows):
                from_ref, place = source(k, r)
                value = from_ref[place, at : at + step, :].astype(jnp.float32) * scale + shift
                half = 0.5 * value
                act = half * jnp.tanh(half) + half
                act = jnp.where(r < length, act, 0.0).astype(jnp.bfloat16)
                a_ref[r + 1, here, :] = act
        a_ref[length + 1, pl.ds(base, local_c), :] = h_refs[k][1]

    lanes = lax.broadcasted_iota(jnp.int32, (local_c, width), 1)
    double = (
        lax.broadcasted_iota(jnp.int32, (width, 2 * width), 0)
        == lax.div(lax.broadcasted_iota(jnp.int32, (width, 2 * width), 1), 2)
    ).astype(jnp.bfloat16)
    per = 2
    for copy in copies[1:]:
        copy.wait()

    def block(b, carry):
        r0 = b * per
        acc = None
        for dy in range(3):
            right = jnp.concatenate([a_ref[r0 + dy + i] for i in range(per)], axis=1)
            part = jnp.dot(w_ref[dy], right, preferred_element_type=jnp.float32)
            acc = part if acc is None else acc + part
        for i in range(per):
            r = r0 + i
            cut = slice(i * width, (i + 1) * width)
            low = acc[:local_c, cut]
            mid = acc[local_c : 2 * local_c, cut]
            high = acc[2 * local_c :, cut]
            low = jnp.where(lanes == 0, 0.0, pltpu.roll(low, 1, 1))
            high = jnp.where(lanes == width - 1, 0.0, pltpu.roll(high, width - 1, 1))
            value = x_ref[r].astype(jnp.float32) + (mid + low + high)
            value = jnp.where(r < length, value, 0.0).astype(jnp.bfloat16)
            wide = jnp.dot(value, double, preferred_element_type=jnp.float32)
            o_ref[r] = wide.astype(jnp.bfloat16)
            for a in range(2):
                pltpu.make_async_copy(o_ref.at[r], out_ref.at[2 * r + a], sem).start()
        return carry

    lax.fori_loop(0, rows // per, block, 0)
    for r in range(rows):
        for a in range(2):
            pltpu.make_async_copy(o_ref.at[r], out_ref.at[2 * r + a], sem).wait()


def pairs(count, k):
    return [(i, i ^ k) for i in range(count)]


def per_device(
    activations,
    weight,
    gamma,
    beta,
    group_map,
    lengths,
    stale_edges,
    stale_mean,
    stale_square,
    old_mean,
    old_square,
):
    rows, width, local_c = activations.shape
    taps, channels, _ = weight.shape
    groups = stale_mean.shape[0]
    per_group = channels // groups
    n_chan, n_strip = lax.axis_size("chan"), lax.axis_size("strip")
    me, strip = lax.axis_index("chan"), lax.axis_index("strip")
    total = float(n_strip * (3 * rows // 4) * width * per_group)
    x = jnp.swapaxes(activations, 1, 2)
    w = jnp.swapaxes(weight, 1, 2).reshape(3, 3 * local_c, channels)
    edges = jnp.swapaxes(stale_edges, 1, 2)
    gm = group_map.reshape(1, channels)
    where = jnp.stack(
        [lengths[0], me.astype(jnp.int32), lax.rem(strip, 2).astype(jnp.int32), strip.astype(jnp.int32), jnp.int32(n_strip)]
    )
    early = EARLY
    bf16, f32 = jnp.bfloat16, jnp.float32
    row = (local_c, width)

    def shape(n):
        return jax.ShapeDtypeStruct((n, *row), bf16)

    def chan(value, k):
        return lax.ppermute(value, "chan", pairs(n_chan, k))

    sums = jax.ShapeDtypeStruct((groups, 128), f32)
    head, tail, near_out, part = pl.pallas_call(
        functools.partial(stats_kernel, n_chan, groups),
        out_shape=(shape(early + 1), shape(rows - early), shape(2), sums),
        in_specs=[spec(pltpu.SMEM), spec(), spec(pl.ANY), spec(pl.ANY)],
        out_specs=(spec(),) * 4,
        scratch_shapes=[
            VMEM((rows, *row), bf16),
            VMEM((local_c, 2 * width), f32),
            pltpu.SemaphoreType.DMA((2,)),
        ],
        compiler_params=pltpu.CompilerParams(vmem_limit_bytes=8 * MIB),
        name="stats",
    )(where, gm, x, edges)
    heads = {1: chan(head, 1), 2: chan(head, 2)}
    tails = {1: chan(tail, 1), 2: chan(tail, 2)}
    heads[3] = chan(heads[2], 1)
    tails[3] = chan(tails[2], 1)

    near = lax.ppermute(near_out, "strip", pairs(n_strip, 1))
    far_out, pair = pl.pallas_call(
        far_kernel,
        out_shape=(shape(2), sums),
        in_specs=[spec(pltpu.SMEM), spec(), spec(), spec(pl.ANY)],
        out_specs=(spec(),) * 2,
        scratch_shapes=[pltpu.SemaphoreType.DMA],
        compiler_params=pltpu.CompilerParams(vmem_limit_bytes=4 * MIB),
        name="farmsg",
    )(where, near, part, edges)
    ring = [(i, (((i + 1) ^ 1) - 1) % n_strip) for i in range(n_strip)]
    far = lax.ppermute(far_out, "strip", ring)
    mine = pair + sum(far[1, i * groups : (i + 1) * groups].astype(f32) for i in range(3))
    k = 4
    other = lax.ppermute(mine, "strip", pairs(n_strip, k))
    while 2 * k < n_strip:
        k *= 2
        mine = mine + other
        other = lax.ppermute(mine, "strip", pairs(n_strip, k))
    halo = pl.pallas_call(
        halo_kernel,
        out_shape=shape(3),
        in_specs=[spec(pltpu.SMEM)] + [spec()] * 4,
        out_specs=spec(),
        compiler_params=pltpu.CompilerParams(vmem_limit_bytes=4 * MIB),
        name="halo",
    )(where, near, far, mine, other)
    halos = [halo, chan(halo, 1), chan(halo, 2)]
    halos.append(chan(halos[2], 1))

    out, new_mean, new_square = pl.pallas_call(
        functools.partial(conv_kernel, n_chan, per_group, total),
        out_shape=(
            jax.ShapeDtypeStruct((2 * rows, local_c, 2 * width), bf16),
            jax.ShapeDtypeStruct((1, groups), f32),
            jax.ShapeDtypeStruct((1, groups), f32),
        ),
        in_specs=[spec(pltpu.SMEM)] + [spec()] * 8 + [spec(pl.ANY)] * 2 + [spec()] * (3 * n_chan - 2),
        out_specs=(spec(pl.ANY), spec(), spec()),
        scratch_shapes=[
            VMEM((rows, *row), bf16),
            VMEM((3, 3 * local_c, channels), bf16),
            VMEM((rows + 2, channels, width), bf16),
            VMEM((channels, 2 * width), f32),
            VMEM((rows, local_c, 2 * width), bf16),
            pltpu.SemaphoreType.DMA,
            pltpu.SemaphoreType.DMA((4,)),
        ],
        compiler_params=pltpu.CompilerParams(vmem_limit_bytes=32 * MIB),
        cost_estimate=pl.CostEstimate(
            flops=2 * rows * width * taps * channels * local_c,
            bytes_accessed=taps * channels * local_c * 2,
            transcendentals=rows * width * channels,
        ),
        name="conv",
    )(
        where,
        part,
        stale_mean.reshape(1, groups),
        stale_square.reshape(1, groups),
        old_mean,
        old_square,
        gm,
        gamma.reshape(1, channels),
        beta.reshape(1, channels),
        x,
        w,
        *[heads[k] for k in range(1, n_chan)],
        *[tails[k] for k in range(1, n_chan)],
        *halos,
    )
    upsampled = jnp.swapaxes(out, 1, 2)
    return (upsampled, new_mean.reshape(groups), new_square.reshape(groups))


def solution(mesh):
    in_specs = (
        P("strip", None, "chan"),
        P(None, None, "chan"),
        P(),
        P(),
        P(),
        P("strip"),
        P("strip", None, "chan"),
        P(),
        P(),
        P("strip", None),
        P("strip", None),
    )
    out_specs = (P("strip", None, "chan"), P(), P())
    return jax.shard_map(
        per_device, mesh=mesh, in_specs=in_specs, out_specs=out_specs, check_vma=False
    )
```
